32 devices in a mesh: expert: 4 (over y, x), dp: 8 (over z, core).
Axes of the slice: x: 2, y: 2, z: 4, core: 2. Of those that a mesh axis runs over, the one named last changes fastest.
Arguments:
- tokens: bfloat16 [2, 4096, 1280], P(None, ('expert', 'dp')), may hold values from -6 to 6
- modality: int32 [2, 4096], P(None, ('expert', 'dp')), may hold values from 0 to 1, as said below
- routes: int32 [2, 4096, 1], P(None, ('expert', 'dp')), may hold values from 0 to 3; in each aligned block of 128 rows (0 to 127, 128 to 255, ..., all dimensions but the last counted through in order) at most 64 rows name the same one
- router: bfloat16 [1280, 4], replicated, may hold values from -0.15625 to 0.15625
- w_in: bfloat16 [4, 1280, 5120], P('expert', 'dp'), may hold values from -0.15625 to 0.15625
- w_out: bfloat16 [4, 5120, 1280], P('expert', 'dp'), may hold values from -0.078125 to 0.078125
Outputs:
- mixed: bfloat16 [2, 4096, 1280], P(None, ('expert', 'dp'))
- load: float32 [2, 2, 4], replicated
The draws below stay inside these ranges and needn't reach their ends.
Inputs may be any that keep to these rules, and one draw needn't show every extreme that they name: `routes`: among the 128 tokens of one micro-batch on one device (aligned blocks of 128 rows), at most 64 are routed to any one expert. `modality`: in every aligned block of 128 tokens of a micro-batch, the number of text tokens lies between 32 and 96.
All inputs are finite; a program needn't handle non-finite values.
Results may differ from the reference program's by a relative error of at most 0.0057.
Values may be sent and summed in bfloat16 or wider, within the bound.
A program may use at most 192 MiB of HBM per device.

```python
import math
import jax
import jax.numpy as jnp
import numpy as np
from jax import lax

D = 1280
FF = 5120
MB = 2
TOK_MB = 128
EXPERTS = 4
CAP = 64
TOKENS = 4096


def draw_modality(key, part):
    n_blocks = TOKENS // TOK_MB
    scores = jax.random.randint(key, (MB, n_blocks, TOK_MB), 0, 1 << 20) * TOK_MB + jnp.arange(TOK_MB, dtype=jnp.int32)
    order = jnp.argsort(scores, axis=-1)
    ranked = jnp.argsort(order, axis=-1)
    texts = TOK_MB // 4 + TOK_MB // 2 * jnp.arange(n_blocks, dtype=jnp.int32) // max(n_blocks - 1, 1)
    return (ranked < texts[None, :, None]).astype(jnp.int32).reshape(MB, TOKENS)


def level_of(key, shape, cuts, least, largest):
    def one(axis_at, shards_of):
        heights = jax.random.uniform(jax.random.fold_in(jax.random.fold_in(key, 6), axis_at), (shards_of,), jnp.float32, least / len(cuts), largest / len(cuts))
        return jnp.repeat(jnp.exp(heights), shape[axis_at] // shards_of).reshape((-1,) + (1,) * (len(shape) - axis_at - 1))

    gain = one(*cuts[0])
    for cut in cuts[1:]:
        gain = gain * one(*cut)
    return gain


def shared_out(key, own, number, rows, count, top, reach, skew):
    order = jax.random.permutation(key, count)
    crowded, common = load_shares(count, rows * top, reach, skew, True), load_shares(count, rows * top, reach, skew, False)
    places = jnp.arange(count)

    def named(sizes, offset_by):
        used = int((sizes > 0).sum())
        fixed = max(1, used // 4)
        shifted = fixed + (places - fixed + offset_by * (used - fixed)) % max(1, count - fixed)
        return jnp.zeros((count,), jnp.int32).at[order[jnp.where(places < fixed, places, shifted)]].set(jnp.asarray(sizes, jnp.int32))

    sizes = jnp.where(number % 4 == 0, named(crowded, number // 4), named(common, number - number // 4 - 1))
    mixed = jax.random.permutation(jax.random.fold_in(own, 3), count)
    donor, sink = mixed[0:count // 2 * 2:2], mixed[1:count // 2 * 2:2]
    room = jnp.minimum(sizes[donor] - 1, reach - sizes[sink]) // 2
    room = jnp.where((donor == order[0]) | (sink == order[0]) | (sizes[sink] == 0), 0, jnp.maximum(room, 0))
    shifted = jax.random.randint(jax.random.fold_in(own, 4), (count // 2,), 0, 1 << 20) % (room + 1)
    sizes = sizes.at[donor].add(-shifted).at[sink].add(shifted)
    items = jnp.searchsorted(jnp.cumsum(sizes), jnp.arange(rows * top), side="right").astype(jnp.int32)
    listing = items.reshape(top, rows).T
    listing = listing[jax.random.permutation(jax.random.fold_in(own, 1), rows)]
    offset_by = jax.random.randint(jax.random.fold_in(own, 2), (rows, 1), 0, top)
    return jnp.take_along_axis(listing, (jnp.arange(top)[None, :] + offset_by) % top, axis=1)


def load_shares(number_of, total, most, skew, full):
    portions = [(1 << 20) // math.isqrt(grade ** skew) + 1 for grade in range(1, number_of + 1)]
    largest = most if full else min(most, max(-(-total // number_of), total * portions[0] // sum(portions)))
    least = 1 if total - largest >= number_of - 1 else 0
    given, rest = [largest] + [least] * (number_of - 1), total - largest - least * (number_of - 1)
    while rest > 0:
        candidates = [i for i in range(1, number_of) if given[i] < largest] or [i for i in range(1, number_of) if given[i] < most]
        pool, budget = sum([portions[i] for i in candidates]), rest
        for i in candidates:
            extra = min(most - given[i], max(1, budget * portions[i] // pool), rest)
            given[i] = given[i] + extra
            rest = rest - extra
    return np.array(given)


def gaussian(stream_key, shape, deviation, reach, pieces=(), kind=jnp.bfloat16):
    drawn = jax.random.normal(stream_key, shape, jnp.float32) * deviation
    if len(pieces) > 0:
        drawn = level_of(stream_key, shape, pieces, -0.22, 0.18) * drawn
    return jnp.clip(drawn, min=-reach, max=reach).astype(kind)


def setup_inputs(seed: int = 0) -> dict:
    streams_of = jax.random.split(jax.random.key(seed), 7)
    tokens = gaussian(streams_of[0], (MB, TOKENS, D), 1.0, 6.0, ((1, 32),))
    modality = draw_modality(jax.random.fold_in(streams_of[6], 71), 0)
    routes_keys = jax.random.split(jax.random.fold_in(streams_of[2], 1), MB * TOKENS // TOK_MB)
    routes_turns = jax.random.permutation(jax.random.fold_in(streams_of[2], 3), MB * TOKENS // TOK_MB)
    routes = jax.vmap(lambda own, number: shared_out(jax.random.fold_in(streams_of[2], 2), own, number, TOK_MB, EXPERTS, 1, CAP, 2))(routes_keys, routes_turns).reshape((MB, TOKENS, 1))
    router = gaussian(streams_of[3], (D, EXPERTS), D ** -0.5, 0.15625)
    w_in = gaussian(streams_of[4], (EXPERTS, D, FF), D ** -0.5, 0.15625, ((0, 4), (1, 8)))
    w_out = gaussian(streams_of[5], (EXPERTS, FF, D), FF ** -0.5, 0.078125, ((0, 4), (1, 8)))
    return dict(tokens=tokens, modality=modality, routes=routes, router=router, w_in=w_in, w_out=w_out)


def expert_mlp(operands):
    rows_in, weight_in, weight_out = operands
    pre_act = jnp.dot(rows_in, weight_in, preferred_element_type=jnp.float32)
    hidden = jax.nn.gelu(pre_act, approximate=True).astype(jnp.bfloat16)
    return jnp.dot(hidden, weight_out, preferred_element_type=jnp.float32).astype(jnp.bfloat16)


def reference(tokens, modality, routes, router, w_in, w_out):
    blocks = TOKENS // TOK_MB
    slot_bound = blocks * CAP
    mixed_list = []
    counts = jnp.zeros((2, EXPERTS), jnp.float32)
    prob_sums = jnp.zeros((2, EXPERTS), jnp.float32)
    modal_counts = jnp.zeros((2,), jnp.float32)
    for micro in range(MB):
        micro_tokens = tokens[micro]
        expert_ids = routes[micro, :, 0].astype(jnp.int32)
        logits = jnp.dot(micro_tokens, router, preferred_element_type=jnp.float32)
        onehot = (expert_ids[:, None] == jnp.arange(EXPERTS, dtype=jnp.int32)[None, :]).astype(jnp.float32)
        gating = jax.nn.sigmoid(jnp.sum(logits * onehot, axis=-1))
        running = jnp.cumsum(onehot.reshape(blocks, TOK_MB, EXPERTS), axis=1).reshape(TOKENS, EXPERTS)
        slot_pos = (jnp.sum(running * onehot, axis=-1) - 1.0).astype(jnp.int32)
        device = (jnp.arange(TOKENS, dtype=jnp.int32) // TOK_MB).astype(jnp.int32)
        position = (expert_ids * slot_bound + device * CAP + slot_pos).astype(jnp.int32)
        buffer = jnp.zeros((EXPERTS * slot_bound, D), jnp.bfloat16).at[position].set(micro_tokens)
        buffer = buffer.reshape(EXPERTS, slot_bound, D)
        result = lax.map(expert_mlp, (buffer, w_in, w_out)).reshape(EXPERTS * slot_bound, D)
        scaled = result[position].astype(jnp.float32) * gating[:, None]
        mixed_list.append(scaled.astype(jnp.bfloat16))
        exps = jnp.exp(logits)
        router_probs = exps / jnp.sum(exps, axis=-1, keepdims=True)
        modal_hot = (modality[micro][:, None] == jnp.arange(2, dtype=jnp.int32)[None, :]).astype(jnp.float32)
        counts = counts + jnp.dot(modal_hot.T, onehot, precision=lax.Precision.HIGHEST)
        prob_sums = prob_sums + jnp.dot(modal_hot.T, router_probs, precision=lax.Precision.HIGHEST)
        modal_counts = modal_counts + jnp.sum(modal_hot, axis=0)
    load = jnp.stack([EXPERTS * counts / modal_counts[:, None], EXPERTS * prob_sums / modal_counts[:, None]])
    return jnp.stack(mixed_list), load
```

```python
import jax
import jax.numpy as jnp
from jax import lax
from jax.sharding import PartitionSpec as P


def on_device(tokens, modality, routes, router, w_in, w_out):
    micro_count, tok_count, model_width = tokens.shape
    experts = router.shape[1]
    capacity = 2 * tok_count // experts
    ranks = lax.axis_size("dp")
    half = ranks // 2
    upper = lax.axis_index("dp") >= half
    swap = [(i, (i + half) % ranks) for i in range(ranks)]
    groups = [list(range(half)), list(range(half, ranks))]

    other_tokens = lax.ppermute(tokens, "dp", swap)
    other_routes = lax.ppermute(routes, "dp", swap)
    half_ff = w_in.shape[2] // 2
    lower_cols, upper_cols = w_in[0, :, :half_ff], w_in[0, :, half_ff:]
    kept = jnp.where(upper, upper_cols, lower_cols)
    given = lax.ppermute(jnp.where(upper, lower_cols, upper_cols), "dp", swap)
    near_in = lax.all_gather(kept, "dp", axis=0, tiled=True, axis_index_groups=groups)
    far_in = lax.all_gather(given, "dp", axis=0, tiled=True, axis_index_groups=groups)
    part_out = lax.all_gather(w_out[0], "dp", axis=0, tiled=True, axis_index_groups=groups)

    logits = jnp.einsum("mtd,de->mte", tokens, router, preferred_element_type=jnp.float32)
    both_tokens = jnp.concatenate([tokens, other_tokens])
    both_routes = jnp.concatenate([routes, other_routes])
    onehot = (both_routes == jnp.arange(experts, dtype=jnp.int32)[None, None, :]).astype(
        jnp.float32
    )
    running = jnp.cumsum(onehot, axis=1)
    slot_pos = jnp.sum((running - 1.0) * onehot, axis=-1)
    slot_hot = (
        slot_pos[:, :, None] == jnp.arange(capacity, dtype=jnp.float32)[None, None, :]
    ).astype(jnp.float32)
    placer = (onehot[:, :, :, None] * slot_hot[:, :, None, :]).reshape(
        2 * micro_count, tok_count, experts * capacity
    )
    placer = placer.astype(jnp.bfloat16)
    onehot = onehot[:micro_count]
    gating = jax.nn.sigmoid(jnp.sum(logits * onehot, axis=-1))

    buffer = jnp.einsum("mtk,mtd->kmd", placer, both_tokens, preferred_element_type=jnp.float32)
    buffer = buffer.astype(jnp.bfloat16).reshape(experts, capacity, 2 * micro_count, model_width)
    buffer = buffer.transpose(0, 2, 1, 3)
    arrived = lax.all_to_all(buffer, "expert", split_axis=0, concat_axis=0, tiled=True)
    rows = arrived.reshape(-1, model_width)
    mid = model_width // 2
    near_rows = jnp.where(upper, rows[:, mid:], rows[:, :mid])
    far_rows = jnp.where(upper, rows[:, :mid], rows[:, mid:])
    pre_act = jnp.dot(near_rows, near_in, preferred_element_type=jnp.float32)
    pre_act = pre_act + jnp.dot(far_rows, far_in, preferred_element_type=jnp.float32)
    hidden = jax.nn.gelu(pre_act, approximate=True).astype(jnp.bfloat16)
    hidden = hidden.reshape(experts, 2 * micro_count, capacity, half_ff)

    def served(first):
        mine = hidden[:, first : first + micro_count]
        out = jnp.dot(
            mine.reshape(-1, half_ff), part_out, preferred_element_type=jnp.float32
        ).astype(jnp.bfloat16)
        out = out.reshape(experts, micro_count, capacity, model_width)
        back = lax.all_to_all(out, "expert", split_axis=0, concat_axis=0, tiled=True)
        back = back.transpose(1, 0, 2, 3).reshape(micro_count, experts * capacity, model_width)
        return jnp.einsum(
            "mtk,mkd->mtd",
            placer[first : first + micro_count],
            back,
            preferred_element_type=jnp.float32,
        )

    sent = lax.ppermute(served(micro_count).astype(jnp.bfloat16), "dp", swap)
    combined = served(0) + sent.astype(jnp.float32)
    mixed = (combined * gating[:, :, None]).astype(jnp.bfloat16)

    exps = jnp.exp(logits)
    router_probs = exps / jnp.sum(exps, axis=-1, keepdims=True)
    modal_hot = (modality[:, :, None] == jnp.arange(2, dtype=jnp.int32)[None, None, :]).astype(
        jnp.float32
    )
    counts = jnp.einsum("mtk,mte->ke", modal_hot, onehot, precision=lax.Precision.HIGHEST)
    prob_sums = jnp.einsum("mtk,mte->ke", modal_hot, router_probs, precision=lax.Precision.HIGHEST)
    modal_counts = jnp.sum(modal_hot, axis=(0, 1))
    sums = jnp.concatenate([counts, prob_sums, modal_counts[:, None]], axis=1)
    sums = lax.psum(sums, ("expert", "dp"))
    counts, prob_sums = sums[:, :experts], sums[:, experts : 2 * experts]
    modal_counts = sums[:, 2 * experts :]
    load = jnp.stack([experts * counts / modal_counts, experts * prob_sums / modal_counts])
    return (mixed, load)


def solution(mesh):
    placed = (
        P(None, ("expert", "dp"), None),
        P(None, ("expert", "dp")),
        P(None, ("expert", "dp"), None),
        P(),
        P("expert", "dp", None),
        P("expert", "dp", None),
    )
    return jax.shard_map(
        on_device,
        mesh=mesh,
        in_specs=placed,
        out_specs=(P(None, ("expert", "dp"), None), P()),
        check_vma=False,
    )
```

```python
import functools

import jax
import jax.numpy as jnp
from jax import lax
from jax.experimental import pallas as pl
from jax.experimental.pallas import tpu as pltpu
from jax.sharding import PartitionSpec as P

MESH = pl.DeviceIdType.MESH


def layer_kernel(
    experts,
    ranks,
    tokens_ref,
    slots_ref,
    gating_ref,
    sums_ref,
    w_in_ref,
    w_out_ref,
    mixed_ref,
    total_ref,
    tok_far,
    slots_far,
    stats,
    win,
    wout,
    xs,
    xr,
    acc,
    hid,
    ys,
    yr,
    zs,
    zr,
    stat_sem,
    tok_sem,
    slot_sem,
    in_sem,
    out_sem,
    x_sem,
    y_sem,
    z_sem,
):
    micro, tok, width = tokens_ref.shape
    in_rows, ff = w_in_ref.shape
    out_rows = w_out_ref.shape[0]
    half_ff = ff // 2
    cap = xs.shape[3]
    slots_all = experts * cap
    e = lax.axis_index("expert")
    p = lax.axis_index("dp")
    z, c = p // 2, p % 2
    chips = ranks // 2
    group = chips // 2
    h = z // group
    zl = z % group
    partner = ((z + group) % chips) * 2 + c
    mate = z * 2 + (1 - c)
    me = e * ranks + p
    total = experts * ranks

    barrier = pltpu.get_barrier_semaphore()

    def greet(k, carry):
        t = (me + k) % total
        pl.semaphore_signal(
            barrier, inc=1, device_id=(t // ranks, t % ranks), device_id_type=MESH
        )
        return carry

    lax.fori_loop(1, total, greet, 0)

    def remote(src, dst, sems, at, dp=None, expert=None):
        return pltpu.make_async_remote_copy(
            src_ref=src,
            dst_ref=dst,
            send_sem=sems.at[(0,) + at],
            recv_sem=sems.at[(1,) + at],
            device_id=(e if expert is None else expert, p if dp is None else dp),
            device_id_type=MESH,
        )

    def win_rows(q):
        return win.at[pl.ds(pl.multiple_of(q * in_rows, 16), in_rows), :]

    def wout_rows(q, piece):
        size = out_rows // 2
        return wout.at[pl.ds(pl.multiple_of(q * out_rows + piece * size, 16), size), :]

    def cols(which):
        return w_in_ref.at[:, pl.ds(pl.multiple_of(which * half_ff, 128), half_ff)]

    def peer(k):
        return (h * group + (zl + k) % group) * 2 + c

    def place(k):
        return ((zl + k) % group) * 2 + c

    pl.semaphore_wait(barrier, total - 1)

    pending = []

    def go(copy):
        copy.start()
        pending.append(copy)
        return copy

    tok_copy = go(remote(tokens_ref, tok_far, tok_sem, (), dp=partner))
    slot_copy = go(remote(slots_ref, slots_far, slot_sem, (), dp=partner))
    far_copy = go(remote(cols(1 - h), win_rows(p), in_sem, (1, 0, 0), dp=partner))
    near_copies = [
        go(remote(cols(h), win_rows(p), in_sem, (0, 0, k), dp=peer(k))) for k in range(1, group)
    ]
    near_mate = [go(remote(cols(h), win_rows(p), in_sem, (0, 1, 0), dp=mate))]
    own_in = pltpu.make_async_copy(cols(h), win_rows(p), in_sem.at[0, 0, 0, 0])
    own_in.start()

    def send_out(piece):
        size = out_rows // 2
        src = w_out_ref.at[pl.ds(piece * size, size), :]
        dst = wout_rows(place(0), piece)
        peers = [
            go(remote(src, dst, out_sem, (piece, 0, k), dp=peer(k))) for k in range(1, group)
        ]
        mates = [go(remote(src, dst, out_sem, (piece, 1, 0), dp=mate))]
        own = pltpu.make_async_copy(src, dst, out_sem.at[0, piece, 0, 0])
        own.start()
        return peers, mates, own

    out_first = send_out(0)

    def tell(k, carry):
        t = (me + k) % total
        pltpu.make_async_remote_copy(
            src_ref=sums_ref,
            dst_ref=stats.at[me],
            send_sem=stat_sem.at[0],
            recv_sem=stat_sem.at[1],
            device_id=(t // ranks, t % ranks),
            device_id_type=MESH,
        ).start()
        return carry

    lax.fori_loop(1, total, tell, 0)

    def placer_of(ref, m):
        hot = lax.broadcasted_iota(jnp.int32, (slots_all, tok), 0) == ref[m, 0:1, :]
        return jnp.where(hot, 1.0, 0.0).astype(jnp.bfloat16)

    def dispatch(side, tok_ref, slot_ref):
        for m in range(micro):
            put = jnp.dot(
                placer_of(slot_ref, m), tok_ref[m], preferred_element_type=jnp.float32
            ).astype(jnp.bfloat16)
            for to in range(experts):
                xs[side, to, m] = put[to * cap : (to + 1) * cap]
        copies = [
            go(
                remote(
                    xs.at[side, (e + k) % experts],
                    xr.at[side, e],
                    x_sem,
                    (side, k),
                    expert=(e + k) % experts,
                )
            )
            for k in range(1, experts)
        ]
        own = pltpu.make_async_copy(xs.at[side, e], xr.at[side, e], x_sem.at[0, side, 0])
        own.start()
        return copies, own

    def landed(copies, own):
        for copy in copies:
            copy.wait_recv()
        own.wait()

    own_x = dispatch(0, tokens_ref, slots_ref)
    tok_copy.wait_recv()
    slot_copy.wait_recv()
    far_x = dispatch(1, tok_far, slots_far)

    for k, copy in zip(range(1, group), near_copies):
        copy.wait_recv()
        rows = win_rows(peer(group - k))
        near_mate.append(go(remote(rows, rows, in_sem, (0, 1, k), dp=mate)))

    landed(*own_x)
    landed(*far_x)
    own_in.wait()
    for copy in near_mate:
        copy.wait_recv()

    side_rows = experts * micro * cap
    tile = 512 if half_ff % 512 == 0 else 128
    half_w = width // 2

    def first_dot(side, which, at):
        left = xr[side, :, :, :, pl.ds(pl.multiple_of(which * half_w, 128), half_w)]
        right = win[pl.ds(pl.multiple_of(which * half_w, 16), half_w), pl.ds(at, tile)]
        return jnp.dot(
            left.reshape(side_rows, half_w), right, preferred_element_type=jnp.float32
        )

    def near_tile(i, carry):
        at = pl.multiple_of(i * tile, 128)
        for side in range(2):
            acc[side, :, pl.ds(at, tile)] = first_dot(side, h, at)
        return carry

    far_copy.wait_recv()
    rows = win_rows(partner)
    far_copies = [
        go(remote(rows, rows, in_sem, (1, 0, k), dp=peer(k))) for k in range(1, group)
    ]
    far_mate = [go(remote(rows, rows, in_sem, (1, 1, 0), dp=mate))]
    out_second = send_out(1)

    lax.fori_loop(0, half_ff // tile, near_tile, 0)

    for k, copy in zip(range(1, group), far_copies):
        copy.wait_recv()
        source = (((z + group) % chips) // group) * group + (zl + group - k) % group
        rows = win_rows(source * 2 + c)
        far_mate.append(go(remote(rows, rows, in_sem, (1, 1, k), dp=mate)))
    for copy in far_mate:
        copy.wait_recv()

    def far_tile(i, carry):
        at = pl.multiple_of(i * tile, 128)
        for side in range(2):
            pre = acc[side, :, pl.ds(at, tile)] + first_dot(side, 1 - h, at)
            hid[side, :, pl.ds(at, tile)] = jax.nn.gelu(pre, approximate=True).astype(
                jnp.bfloat16
            )
        return carry

    lax.fori_loop(0, half_ff // tile, far_tile, 0)

    out_mates = []
    for piece, (peers, mates, own) in enumerate((out_first, out_second)):
        for k, copy in zip(range(1, group), peers):
            copy.wait_recv()
            rows = wout_rows(place(group - k), piece)
            out_mates.append(go(remote(rows, rows, out_sem, (piece, 1, k), dp=mate)))
        out_mates.extend(mates)
        own.wait()
    for copy in out_mates:
        copy.wait_recv()

    out_tile = 256 if width % 256 == 0 else 128

    def second(side):
        def out_col(i, carry):
            at = pl.multiple_of(i * out_tile, 128)
            got = jnp.dot(
                hid[side], wout[:, pl.ds(at, out_tile)], preferred_element_type=jnp.float32
            ).astype(jnp.bfloat16)
            ys[side, :, :, :, pl.ds(at, out_tile)] = got.reshape(experts, micro, cap, out_tile)
            return carry

        lax.fori_loop(0, width // out_tile, out_col, 0)
        copies = [
            go(
                remote(
                    ys.at[side, (e + k) % experts],
                    yr.at[side, e],
                    y_sem,
                    (side, k),
                    expert=(e + k) % experts,
                )
            )
            for k in range(1, experts)
        ]
        own = pltpu.make_async_copy(ys.at[side, e], yr.at[side, e], y_sem.at[0, side, 0])
        own.start()
        return copies, own

    def combine(side, m, slot_ref):
        back = yr[side, :, m].reshape(slots_all, width)
        return lax.dot_general(
            placer_of(slot_ref, m),
            back,
            (((0,), (0,)), ((), ())),
            preferred_element_type=jnp.float32,
        )

    far_y = second(1)
    landed(*far_y)
    z_copies = []
    for m in range(micro):
        zs[m] = combine(1, m, slots_far).astype(jnp.bfloat16)
        z_copies.append(go(remote(zs.at[m], zr.at[m], z_sem, (m,), dp=partner)))
    own_y = second(0)

    pltpu.make_async_copy(
        stats.at[pl.ds(1, total - 1)], stats.at[pl.ds(1, total - 1)], stat_sem.at[1]
    ).wait()
    pltpu.make_async_copy(
        stats.at[pl.ds(1, total - 1)], stats.at[pl.ds(1, total - 1)], stat_sem.at[0]
    ).wait()
    stats[me] = sums_ref[...]
    total_ref[...] = jnp.sum(stats[...], axis=0)

    landed(*own_y)
    for m in range(micro):
        mine = combine(0, m, slots_ref)
        z_copies[m].wait_recv()
        both = mine + zr[m].astype(jnp.float32)
        mixed_ref[m] = (both * gating_ref[m]).astype(jnp.bfloat16)
    for copy in pending:
        copy.wait_send()


def on_device(tokens, modality, routes, router, w_in, w_out):
    micro, tok, width = tokens.shape
    experts = router.shape[1]
    cap = 2 * tok // experts
    ranks = lax.axis_size("dp")
    group = ranks // 4
    total = experts * ranks
    half_ff = w_in.shape[2] // 2

    logits = jnp.einsum("mtd,de->mte", tokens, router, preferred_element_type=jnp.float32)
    onehot = (routes == jnp.arange(experts, dtype=jnp.int32)[None, None, :]).astype(jnp.float32)
    gating = jax.nn.sigmoid(jnp.sum(logits * onehot, axis=-1, keepdims=True))
    before = jnp.cumsum(onehot, axis=1) - 1.0
    slots = jnp.sum(before * onehot, axis=-1).astype(jnp.int32) + routes[:, :, 0] * cap
    slots = jnp.broadcast_to(slots[:, None, :], (micro, 8, tok))
    exps = jnp.exp(logits)
    router_probs = exps / jnp.sum(exps, axis=-1, keepdims=True)
    modal_hot = (modality[:, :, None] == jnp.arange(2, dtype=jnp.int32)[None, None, :]).astype(
        jnp.float32
    )
    columns = jnp.concatenate([onehot, router_probs, jnp.ones_like(gating)], axis=-1)
    sums = jnp.einsum("mtk,mtc->kc", modal_hot, columns, precision=lax.Precision.HIGHEST)
    sums = jnp.pad(sums, ((0, 6), (0, 128 - sums.shape[1])))

    bf16 = jnp.bfloat16
    dma = pltpu.SemaphoreType.DMA
    vmem = pl.BlockSpec(memory_space=pltpu.VMEM)
    mixed, summed = pl.pallas_call(
        functools.partial(layer_kernel, experts, ranks),
        out_shape=(
            jax.ShapeDtypeStruct(tokens.shape, bf16),
            jax.ShapeDtypeStruct((8, 128), jnp.float32),
        ),
        in_specs=[vmem] * 6,
        out_specs=(vmem, vmem),
        scratch_shapes=[
            pltpu.VMEM((micro, tok, width), bf16),
            pltpu.VMEM((micro, 8, tok), jnp.int32),
            pltpu.VMEM((total, 8, 128), jnp.float32),
            pltpu.VMEM((width, half_ff), bf16),
            pltpu.VMEM((half_ff, width), bf16),
            pltpu.VMEM((2, experts, micro, cap, width), bf16),
            pltpu.VMEM((2, experts, micro, cap, width), bf16),
            pltpu.VMEM((2, experts * micro * cap, half_ff), jnp.float32),
            pltpu.VMEM((2, experts * micro * cap, half_ff), bf16),
            pltpu.VMEM((2, experts, micro, cap, width), bf16),
            pltpu.VMEM((2, experts, micro, cap, width), bf16),
            pltpu.VMEM((micro, tok, width), bf16),
            pltpu.VMEM((micro, tok, width), bf16),
            dma((2,)),
            dma((2,)),
            dma((2,)),
            dma((2, 2, 2, group)),
            dma((2, 2, 2, group)),
            dma((2, 2, experts)),
            dma((2, 2, experts)),
            dma((2, micro)),
        ],
        compiler_params=pltpu.CompilerParams(
            collective_id=0, has_side_effects=True, vmem_limit_bytes=64 * 1024 * 1024 - 65536
        ),
    )(tokens, slots, gating, sums, w_in[0], w_out[0])

    counts, prob_sums = summed[:2, :experts], summed[:2, experts : 2 * experts]
    modal_counts = summed[:2, 2 * experts : 2 * experts + 1]
    load = jnp.stack([experts * counts / modal_counts, experts * prob_sums / modal_counts])
    return (mixed, load)


def solution(mesh):
    placed = (
        P(None, ("expert", "dp"), None),
        P(None, ("expert", "dp")),
        P(None, ("expert", "dp"), None),
        P(),
        P("expert", "dp", None),
        P("expert", "dp", None),
    )
    return jax.shard_map(
        on_device,
        mesh=mesh,
        in_specs=placed,
        out_specs=(P(None, ("expert", "dp"), None), P()),
        check_vma=False,
    )
```

```python
import functools

import jax
import jax.numpy as jnp
from jax import lax
from jax.experimental import pallas as pl
from jax.experimental.pallas import tpu as pltpu
from jax.sharding import PartitionSpec as P

MESH = pl.DeviceIdType.MESH


def layer_kernel(
    experts,
    ranks,
    tokens_ref,
    slots_ref,
    gating_ref,
    sums_ref,
    w_in_ref,
    w_out_ref,
    mixed_ref,
    total_ref,
    tok_far,
    slots_far,
    stats,
    win,
    wout,
    xs,
    xr,
    acc,
    hid,
    ys,
    yr,
    zs,
    zr,
    stat_sem,
    tok_sem,
    slot_sem,
    in_sem,
    out_sem,
    x_sem,
    y_sem,
    z_sem,
):
    micro, tok, width = tokens_ref.shape
    in_rows, ff = w_in_ref.shape
    out_rows = w_out_ref.shape[0]
    half_ff = ff // 2
    pieces, tile_w = zs.shape[0], zs.shape[3]
    cap = xs.shape[3]
    slots_all = experts * cap
    e = lax.axis_index("expert")
    p = lax.axis_index("dp")
    z, c = p // 2, p % 2
    chips = ranks // 2
    group = chips // 2
    h = z // group
    zl = z % group
    partner = ((z + group) % chips) * 2 + c
    mate = z * 2 + (1 - c)
    me = e * ranks + p
    total = experts * ranks

    barrier = pltpu.get_barrier_semaphore()

    def greet(k, carry):
        t = (me + k) % total
        pl.semaphore_signal(
            barrier, inc=1, device_id=(t // ranks, t % ranks), device_id_type=MESH
        )
        return carry

    lax.fori_loop(1, total, greet, 0)

    def remote(src, dst, sems, at, dp=None, expert=None):
        return pltpu.make_async_remote_copy(
            src_ref=src,
            dst_ref=dst,
            send_sem=sems.at[(0,) + at],
            recv_sem=sems.at[(1,) + at],
            device_id=(e if expert is None else expert, p if dp is None else dp),
            device_id_type=MESH,
        )

    def win_rows(q):
        return win.at[pl.ds(pl.multiple_of(q * in_rows, 16), in_rows), :]

    def wout_rows(q, piece):
        return wout.at[
            pl.ds(pl.multiple_of(q * out_rows, 16), out_rows), pl.ds(piece * tile_w, tile_w)
        ]

    def cols(which):
        return w_in_ref.at[:, pl.ds(pl.multiple_of(which * half_ff, 128), half_ff)]

    def peer(k):
        return (h * group + (zl + k) % group) * 2 + c

    def place(k):
        return ((zl + k) % group) * 2 + c

    pl.semaphore_wait(barrier, total - 1)

    pending = []

    def go(copy):
        copy.start()
        pending.append(copy)
        return copy

    tok_copy = go(remote(tokens_ref, tok_far, tok_sem, (), dp=partner))
    slot_copy = go(remote(slots_ref, slots_far, slot_sem, (), dp=partner))
    far_copy = go(remote(cols(1 - h), win_rows(p), in_sem, (1, 0, 0), dp=partner))
    near_copies = [
        go(remote(cols(h), win_rows(p), in_sem, (0, 0, k), dp=peer(k))) for k in range(1, group)
    ]
    near_mate = [go(remote(cols(h), win_rows(p), in_sem, (0, 1, 0), dp=mate))]
    own_in = pltpu.make_async_copy(cols(h), win_rows(p), in_sem.at[0, 0, 0, 0])
    own_in.start()

    def send_out(piece):
        src = w_out_ref.at[:, pl.ds(piece * tile_w, tile_w)]
        dst = wout_rows(place(0), piece)
        peers = [
            go(remote(src, dst, out_sem, (piece, 0, k), dp=peer(k))) for k in range(1, group)
        ]
        mates = [go(remote(src, dst, out_sem, (piece, 1, 0), dp=mate))]
        own = pltpu.make_async_copy(src, dst, out_sem.at[0, piece, 0, 0])
        own.start()
        return peers, mates, own

    early = pieces // 2
    out_sent = [send_out(piece) for piece in range(early)]

    def tell(k, carry):
        t = (me + k) % total
        pltpu.make_async_remote_copy(
            src_ref=sums_ref,
            dst_ref=stats.at[me],
            send_sem=stat_sem.at[0],
            recv_sem=stat_sem.at[1],
            device_id=(t // ranks, t % ranks),
            device_id_type=MESH,
        ).start()
        return carry

    lax.fori_loop(1, total, tell, 0)

    def placer_of(ref, m):
        hot = lax.broadcasted_iota(jnp.int32, (slots_all, tok), 0) == ref[m, 0:1, :]
        return jnp.where(hot, 1.0, 0.0).astype(jnp.bfloat16)

    def dispatch(side, tok_ref, slot_ref):
        for m in range(micro):
            put = jnp.dot(
                placer_of(slot_ref, m), tok_ref[m], preferred_element_type=jnp.float32
            ).astype(jnp.bfloat16)
            for to in range(experts):
                xs[side, to, m] = put[to * cap : (to + 1) * cap]
        copies = [
            go(
                remote(
                    xs.at[side, (e + k) % experts],
                    xr.at[side, e],
                    x_sem,
                    (side, k),
                    expert=(e + k) % experts,
                )
            )
            for k in range(1, experts)
        ]
        own = pltpu.make_async_copy(xs.at[side, e], xr.at[side, e], x_sem.at[0, side, 0])
        own.start()
        return copies, own

    def landed(copies, own):
        for copy in copies:
            copy.wait_recv()
        own.wait()

    own_x = dispatch(0, tokens_ref, slots_ref)
    tok_copy.wait_recv()
    slot_copy.wait_recv()
    far_x = dispatch(1, tok_far, slots_far)

    for k, copy in zip(range(1, group), near_copies):
        copy.wait_recv()
        rows = win_rows(peer(group - k))
        near_mate.append(go(remote(rows, rows, in_sem, (0, 1, k), dp=mate)))

    landed(*own_x)
    landed(*far_x)
    own_in.wait()
    for copy in near_mate:
        copy.wait_recv()

    side_rows = experts * micro * cap
    tile = 512 if half_ff % 512 == 0 else 128
    half_w = width // 2

    def first_dot(side, which, at):
        left = xr[side, :, :, :, pl.ds(pl.multiple_of(which * half_w, 128), half_w)]
        right = win[pl.ds(pl.multiple_of(which * half_w, 16), half_w), pl.ds(at, tile)]
        return jnp.dot(
            left.reshape(side_rows, half_w), right, preferred_element_type=jnp.float32
        )

    def near_tile(i, carry):
        at = pl.multiple_of(i * tile, 128)
        for side in range(2):
            acc[side, :, pl.ds(at, tile)] = first_dot(side, h, at)
        return carry

    far_copy.wait_recv()
    rows = win_rows(partner)
    far_copies = [
        go(remote(rows, rows, in_sem, (1, 0, k), dp=peer(k))) for k in range(1, group)
    ]
    far_mate = [go(remote(rows, rows, in_sem, (1, 1, 0), dp=mate))]
    out_sent += [send_out(piece) for piece in range(early, pieces)]

    lax.fori_loop(0, half_ff // tile, near_tile, 0)

    for k, copy in zip(range(1, group), far_copies):
        copy.wait_recv()
        source = (((z + group) % chips) // group) * group + (zl + group - k) % group
        rows = win_rows(source * 2 + c)
        far_mate.append(go(remote(rows, rows, in_sem, (1, 1, k), dp=mate)))
    for copy in far_mate:
        copy.wait_recv()

    def far_tile(i, carry):
        at = pl.multiple_of(i * tile, 128)
        for side in range(2):
            pre = acc[side, :, pl.ds(at, tile)] + first_dot(side, 1 - h, at)
            hid[side, :, pl.ds(at, tile)] = jax.nn.gelu(pre, approximate=True).astype(
                jnp.bfloat16
            )
        return carry

    lax.fori_loop(0, half_ff // tile, far_tile, 0)

    def second(side, piece):
        at = piece * tile_w
        got = jnp.dot(
            hid[side], wout[:, at : at + tile_w], preferred_element_type=jnp.float32
        ).astype(jnp.bfloat16)
        ys[side, piece] = got.reshape(experts, micro, cap, tile_w)
        copies = [
            go(
                remote(
                    ys.at[side, piece, (e + k) % experts],
                    yr.at[side, piece, e],
                    y_sem,
                    (side, piece, k),
                    expert=(e + k) % experts,
                )
            )
            for k in range(1, experts)
        ]
        own = pltpu.make_async_copy(
            ys.at[side, piece, e], yr.at[side, piece, e], y_sem.at[0, side, piece, 0]
        )
        own.start()
        return copies, own

    def combine(side, piece, m, slot_ref):
        back = yr[side, piece, :, m].reshape(slots_all, tile_w)
        return lax.dot_general(
            placer_of(slot_ref, m),
            back,
            (((0,), (0,)), ((), ())),
            preferred_element_type=jnp.float32,
        )

    far_y, own_y, z_copies = [], [], []

    def give_back(piece):
        landed(*far_y[piece])
        for m in range(micro):
            zs[piece, m] = combine(1, piece, m, slots_far).astype(jnp.bfloat16)
        z_copies.append(go(remote(zs.at[piece], zr.at[piece], z_sem, (piece,), dp=partner)))

    for piece, (peers, mates, own) in enumerate(out_sent):
        for k, copy in zip(range(1, group), peers):
            copy.wait_recv()
            rows = wout_rows(place(group - k), piece)
            mates.append(go(remote(rows, rows, out_sem, (piece, 1, k), dp=mate)))
        own.wait()
        for copy in mates:
            copy.wait_recv()
        far_y.append(second(1, piece))
        own_y.append(second(0, piece))
        if piece > 0:
            give_back(piece - 1)
    give_back(pieces - 1)

    everyone = stats.at[pl.ds(1, total - 1)]
    pltpu.make_async_copy(everyone, everyone, stat_sem.at[1]).wait()
    pltpu.make_async_copy(everyone, everyone, stat_sem.at[0]).wait()
    stats[me] = sums_ref[...]
    total_ref[...] = jnp.sum(stats[...], axis=0)

    for piece in range(pieces):
        landed(*own_y[piece])
        mine = [combine(0, piece, m, slots_ref) for m in range(micro)]
        z_copies[piece].wait_recv()
        for m in range(micro):
            both = mine[m] + zr[piece, m].astype(jnp.float32)
            mixed_ref[m, :, piece * tile_w : (piece + 1) * tile_w] = (
                both * gating_ref[m]
            ).astype(jnp.bfloat16)
    for copy in pending:
        copy.wait_send()


def on_device(tokens, modality, routes, router, w_in, w_out):
    micro, tok, width = tokens.shape
    experts = router.shape[1]
    cap = 2 * tok // experts
    ranks = lax.axis_size("dp")
    group = ranks // 4
    total = experts * ranks
    half_ff = w_in.shape[2] // 2
    tile_w = 256 if width % 256 == 0 else 128
    pieces = width // tile_w

    logits = jnp.einsum("mtd,de->mte", tokens, router, preferred_element_type=jnp.float32)
    onehot = (routes == jnp.arange(experts, dtype=jnp.int32)[None, None, :]).astype(jnp.float32)
    gating = jax.nn.sigmoid(jnp.sum(logits * onehot, axis=-1, keepdims=True))
    before = jnp.cumsum(onehot, axis=1) - 1.0
    slots = jnp.sum(before * onehot, axis=-1).astype(jnp.int32) + routes[:, :, 0] * cap
    slots = jnp.broadcast_to(slots[:, None, :], (micro, 8, tok))
    exps = jnp.exp(logits)
    router_probs = exps / jnp.sum(exps, axis=-1, keepdims=True)
    modal_hot = (modality[:, :, None] == jnp.arange(2, dtype=jnp.int32)[None, None, :]).astype(
        jnp.float32
    )
    columns = jnp.concatenate([onehot, router_probs, jnp.ones_like(gating)], axis=-1)
    sums = jnp.einsum("mtk,mtc->kc", modal_hot, columns, precision=lax.Precision.HIGHEST)
    sums = jnp.pad(sums, ((0, 6), (0, 128 - sums.shape[1])))

    bf16 = jnp.bfloat16
    dma = pltpu.SemaphoreType.DMA
    vmem = pl.BlockSpec(memory_space=pltpu.VMEM)
    mixed, summed = pl.pallas_call(
        functools.partial(layer_kernel, experts, ranks),
        out_shape=(
            jax.ShapeDtypeStruct(tokens.shape, bf16),
            jax.ShapeDtypeStruct((8, 128), jnp.float32),
        ),
        in_specs=[vmem] * 6,
        out_specs=(vmem, vmem),
        scratch_shapes=[
            pltpu.VMEM((micro, tok, width), bf16),
            pltpu.VMEM((micro, 8, tok), jnp.int32),
            pltpu.VMEM((total, 8, 128), jnp.float32),
            pltpu.VMEM((width, half_ff), bf16),
            pltpu.VMEM((half_ff, width), bf16),
            pltpu.VMEM((2, experts, micro, cap, width), bf16),
            pltpu.VMEM((2, experts, micro, cap, width), bf16),
            pltpu.VMEM((2, experts * micro * cap, half_ff), jnp.float32),
            pltpu.VMEM((2, experts * micro * cap, half_ff), bf16),
            pltpu.VMEM((2, pieces, experts, micro, cap, tile_w), bf16),
            pltpu.VMEM((2, pieces, experts, micro, cap, tile_w), bf16),
            pltpu.VMEM((pieces, micro, tok, tile_w), bf16),
            pltpu.VMEM((pieces, micro, tok, tile_w), bf16),
            dma((2,)),
            dma((2,)),
            dma((2,)),
            dma((2, 2, 2, group)),
            dma((2, pieces, 2, group)),
            dma((2, 2, experts)),
            dma((2, 2, pieces, experts)),
            dma((2, pieces)),
        ],
        compiler_params=pltpu.CompilerParams(
            collective_id=0, has_side_effects=True, vmem_limit_bytes=64 * 1024 * 1024 - 65536
        ),
    )(tokens, slots, gating, sums, w_in[0], w_out[0])

    counts, prob_sums = summed[:2, :experts], summed[:2, experts : 2 * experts]
    modal_counts = summed[:2, 2 * experts : 2 * experts + 1]
    load = jnp.stack([experts * counts / modal_counts, experts * prob_sums / modal_counts])
    return (mixed, load)


def solution(mesh):
    placed = (
        P(None, ("expert", "dp"), None),
        P(None, ("expert", "dp")),
        P(None, ("expert", "dp"), None),
        P(),
        P("expert", "dp", None),
        P("expert", "dp", None),
    )
    return jax.shard_map(
        on_device,
        mesh=mesh,
        in_specs=placed,
        out_specs=(P(None, ("expert", "dp"), None), P()),
        check_vma=False,
    )
```

```python
import functools

import jax
import jax.numpy as jnp
from jax import lax
from jax.experimental import pallas as pl
from jax.experimental.pallas import tpu as pltpu
from jax.sharding import PartitionSpec as P

MESH = pl.DeviceIdType.MESH


def layer_kernel(
    experts,
    ranks,
    tokens_ref,
    routes_ref,
    modality_ref,
    router_ref,
    w_in_ref,
    w_out_ref,
    mixed_ref,
    total_ref,
    tok_far,
    slots_far,
    stats,
    win,
    wout,
    xs,
    xr,
    acc,
    hid,
    ys,
    yr,
    zs,
    zr,
    slots_ref,
    gating_ref,
    sums_ref,
    stat_sem,
    tok_sem,
    slot_sem,
    in_sem,
    out_sem,
    x_sem,
    y_sem,
    z_sem,
):
    micro, tok, width = tokens_ref.shape
    in_rows, ff = w_in_ref.shape
    out_rows = w_out_ref.shape[0]
    half_ff = ff // 2
    pieces, tile_w = zs.shape[0], zs.shape[3]
    cap = xs.shape[3]
    slots_all = experts * cap
    e = lax.axis_index("expert")
    p = lax.axis_index("dp")
    z, c = p // 2, p % 2
    chips = ranks // 2
    group = chips // 2
    h = z // group
    zl = z % group
    partner = ((z + group) % chips) * 2 + c
    mate = z * 2 + (1 - c)
    me = e * ranks + p
    total = experts * ranks

    barrier = pltpu.get_barrier_semaphore()

    def greet(k, carry):
        t = (me + k) % total
        pl.semaphore_signal(
            barrier, inc=1, device_id=(t // ranks, t % ranks), device_id_type=MESH
        )
        return carry

    lax.fori_loop(1, total, greet, 0)

    def remote(src, dst, sems, at, dp=None, expert=None):
        return pltpu.make_async_remote_copy(
            src_ref=src,
            dst_ref=dst,
            send_sem=sems.at[(0,) + at],
            recv_sem=sems.at[(1,) + at],
            device_id=(e if expert is None else expert, p if dp is None else dp),
            device_id_type=MESH,
        )

    def win_rows(q):
        return win.at[pl.ds(pl.multiple_of(q * in_rows, 16), in_rows), :]

    def wout_rows(q, piece):
        return wout.at[
            pl.ds(pl.multiple_of(q * out_rows, 16), out_rows), pl.ds(piece * tile_w, tile_w)
        ]

    def cols(which):
        return w_in_ref.at[:, pl.ds(pl.multiple_of(which * half_ff, 128), half_ff)]

    def peer(k):
        return (h * group + (zl + k) % group) * 2 + c

    def place(k):
        return ((zl + k) % group) * 2 + c

    pl.semaphore_wait(barrier, total - 1)

    pending = []

    def go(copy):
        copy.start()
        pending.append(copy)
        return copy

    tok_copy = go(remote(tokens_ref, tok_far, tok_sem, (), dp=partner))
    far_copy = go(remote(cols(1 - h), win_rows(p), in_sem, (1, 0, 0), dp=partner))
    near_copies = [
        go(remote(cols(h), win_rows(p), in_sem, (0, 0, k), dp=peer(k))) for k in range(1, group)
    ]
    near_mate = [go(remote(cols(h), win_rows(p), in_sem, (0, 1, 0), dp=mate))]
    own_in = pltpu.make_async_copy(cols(h), win_rows(p), in_sem.at[0, 0, 0, 0])
    own_in.start()

    def send_out(piece):
        src = w_out_ref.at[:, pl.ds(piece * tile_w, tile_w)]
        dst = wout_rows(place(0), piece)
        peers = [
            go(remote(src, dst, out_sem, (piece, 0, k), dp=peer(k))) for k in range(1, group)
        ]
        mates = [go(remote(src, dst, out_sem, (piece, 1, 0), dp=mate))]
        own = pltpu.make_async_copy(src, dst, out_sem.at[0, piece, 0, 0])
        own.start()
        return peers, mates, own

    early = pieces // 2
    out_sent = [send_out(piece) for piece in range(early)]

    pad = sums_ref.shape[0]
    row = lax.broadcasted_iota(jnp.int32, (pad, tok), 0)
    real = row < experts
    earlier = lax.broadcasted_iota(jnp.int32, (tok, tok), 0)
    later = lax.broadcasted_iota(jnp.int32, (tok, tok), 1)
    ahead = jnp.where(earlier < later, 1.0, 0.0).astype(jnp.bfloat16)
    hots = []
    for m in range(micro):
        hot = row == routes_ref[m : m + 1, :]
        hots.append(jnp.where(hot, 1.0, 0.0))
        before = jnp.dot(
            hots[m].astype(jnp.bfloat16), ahead, preferred_element_type=jnp.float32
        )
        slot = jnp.sum(jnp.where(hot, before + (row * cap).astype(jnp.float32), 0.0), axis=0)
        slots_ref[m] = jnp.broadcast_to(slot.astype(jnp.int32)[None, :], (8, tok))
    slot_copy = go(remote(slots_ref, slots_far, slot_sem, (), dp=partner))

    def statistics():
        lane = lax.broadcasted_iota(jnp.int32, (pad, 128), 1)
        block = jnp.zeros((pad, 128), jnp.float32)
        for m in range(micro):
            logits = lax.dot_general(
                router_ref[...],
                tokens_ref[m],
                (((1,), (1,)), ((), ())),
                preferred_element_type=jnp.float32,
            )
            gate = jax.nn.sigmoid(jnp.sum(logits * hots[m], axis=0, keepdims=True))
            gating_ref[m] = jnp.transpose(jnp.broadcast_to(gate, (tok, tok)))
            exps = jnp.where(real, jnp.exp(logits), 0.0)
            probs = exps / jnp.sum(exps, axis=0, keepdims=True)
            for kind in range(2):
                modal = jnp.where(modality_ref[m : m + 1, :] == kind, 1.0, 0.0)
                for at, value in enumerate((hots[m], probs, jnp.ones_like(probs))):
                    part = jnp.sum(value * modal, axis=1, keepdims=True)
                    block = block + jnp.where(lane == 2 * at + kind, part, 0.0)
        sums_ref[...] = block

    def tell(k, carry):
        t = (me + k) % total
        pltpu.make_async_remote_copy(
            src_ref=sums_ref,
            dst_ref=stats.at[me],
            send_sem=stat_sem.at[0],
            recv_sem=stat_sem.at[1],
            device_id=(t // ranks, t % ranks),
            device_id_type=MESH,
        ).start()
        return carry

    def placer_of(ref, m):
        hot = lax.broadcasted_iota(jnp.int32, (slots_all, tok), 0) == ref[m, 0:1, :]
        return jnp.where(hot, 1.0, 0.0).astype(jnp.bfloat16)

    def dispatch(side, tok_ref, slot_ref):
        for m in range(micro):
            put = jnp.dot(
                placer_of(slot_ref, m), tok_ref[m], preferred_element_type=jnp.float32
            ).astype(jnp.bfloat16)
            for to in range(experts):
                xs[side, to, m] = put[to * cap : (to + 1) * cap]
        copies = [
            go(
                remote(
                    xs.at[side, (e + k) % experts],
                    xr.at[side, e],
                    x_sem,
                    (side, k),
                    expert=(e + k) % experts,
                )
            )
            for k in range(1, experts)
        ]
        own = pltpu.make_async_copy(xs.at[side, e], xr.at[side, e], x_sem.at[0, side, 0])
        own.start()
        return copies, own

    def landed(copies, own):
        for copy in copies:
            copy.wait_recv()
        own.wait()

    own_x = dispatch(0, tokens_ref, slots_ref)
    statistics()
    lax.fori_loop(1, total, tell, 0)
    tok_copy.wait_recv()
    slot_copy.wait_recv()
    far_x = dispatch(1, tok_far, slots_far)

    for k, copy in zip(range(1, group), near_copies):
        copy.wait_recv()
        rows = win_rows(peer(group - k))
        near_mate.append(go(remote(rows, rows, in_sem, (0, 1, k), dp=mate)))

    landed(*own_x)
    landed(*far_x)
    own_in.wait()
    for copy in near_mate:
        copy.wait_recv()

    side_rows = experts * micro * cap
    tile = 512 if half_ff % 512 == 0 else 128
    half_w = width // 2

    def first_dot(side, which, at):
        left = xr[side, :, :, :, pl.ds(pl.multiple_of(which * half_w, 128), half_w)]
        right = win[pl.ds(pl.multiple_of(which * half_w, 16), half_w), pl.ds(at, tile)]
        return jnp.dot(
            left.reshape(side_rows, half_w), right, preferred_element_type=jnp.float32
        )

    def near_tile(i, carry):
        at = pl.multiple_of(i * tile, 128)
        for side in range(2):
            acc[side, :, pl.ds(at, tile)] = first_dot(side, h, at)
        return carry

    far_copy.wait_recv()
    rows = win_rows(partner)
    far_copies = [
        go(remote(rows, rows, in_sem, (1, 0, k), dp=peer(k))) for k in range(1, group)
    ]
    far_mate = [go(remote(rows, rows, in_sem, (1, 1, 0), dp=mate))]
    out_sent += [send_out(piece) for piece in range(early, pieces)]

    lax.fori_loop(0, half_ff // tile, near_tile, 0)

    for k, copy in zip(range(1, group), far_copies):
        copy.wait_recv()
        source = (((z + group) % chips) // group) * group + (zl + group - k) % group
        rows = win_rows(source * 2 + c)
        far_mate.append(go(remote(rows, rows, in_sem, (1, 1, k), dp=mate)))
    for copy in far_mate:
        copy.wait_recv()

    def far_tile(i, carry):
        at = pl.multiple_of(i * tile, 128)
        for side in range(2):
            pre = acc[side, :, pl.ds(at, tile)] + first_dot(side, 1 - h, at)
            hid[side, :, pl.ds(at, tile)] = jax.nn.gelu(pre, approximate=True).astype(
                jnp.bfloat16
            )
        return carry

    lax.fori_loop(0, half_ff // tile, far_tile, 0)

    def second(side, piece):
        at = piece * tile_w
        got = jnp.dot(
            hid[side], wout[:, at : at + tile_w], preferred_element_type=jnp.float32
        ).astype(jnp.bfloat16)
        ys[side, piece] = got.reshape(experts, micro, cap, tile_w)
        copies = [
            go(
                remote(
                    ys.at[side, piece, (e + k) % experts],
                    yr.at[side, piece, e],
                    y_sem,
                    (side, piece, k),
                    expert=(e + k) % experts,
                )
            )
            for k in range(1, experts)
        ]
        own = pltpu.make_async_copy(
            ys.at[side, piece, e], yr.at[side, piece, e], y_sem.at[0, side, piece, 0]
        )
        own.start()
        return copies, own

    def combine(side, piece, m, slot_ref):
        back = yr[side, piece, :, m].reshape(slots_all, tile_w)
        return lax.dot_general(
            placer_of(slot_ref, m),
            back,
            (((0,), (0,)), ((), ())),
            preferred_element_type=jnp.float32,
        )

    far_y, own_y, z_copies = [], [], []

    def give_back(piece):
        landed(*far_y[piece])
        for m in range(micro):
            zs[piece, m] = combine(1, piece, m, slots_far).astype(jnp.bfloat16)
        z_copies.append(go(remote(zs.at[piece], zr.at[piece], z_sem, (piece,), dp=partner)))

    for piece, (peers, mates, own) in enumerate(out_sent):
        for k, copy in zip(range(1, group), peers):
            copy.wait_recv()
            rows = wout_rows(place(group - k), piece)
            mates.append(go(remote(rows, rows, out_sem, (piece, 1, k), dp=mate)))
        own.wait()
        for copy in mates:
            copy.wait_recv()
        far_y.append(second(1, piece))
        own_y.append(second(0, piece))
        if piece > 0:
            give_back(piece - 1)
    give_back(pieces - 1)

    everyone = stats.at[pl.ds(1, total - 1)]
    pltpu.make_async_copy(everyone, everyone, stat_sem.at[1]).wait()
    pltpu.make_async_copy(everyone, everyone, stat_sem.at[0]).wait()
    stats[me] = sums_ref[...]
    summed = jnp.sum(stats[...], axis=0)
    loads = []
    for at in range(4):
        modal = summed[:, 4 + at % 2 : 5 + at % 2]
        loads.append(experts * summed[:, at : at + 1] / modal)
    lane = lax.broadcasted_iota(jnp.int32, (pad, 128), 1)
    block = jnp.zeros((pad, 128), jnp.float32)
    for at in range(4):
        block = block + jnp.where(lane == at, loads[at], 0.0)
    total_ref[...] = block

    for piece in range(pieces):
        landed(*own_y[piece])
        mine = [combine(0, piece, m, slots_ref) for m in range(micro)]
        z_copies[piece].wait_recv()
        for m in range(micro):
            both = mine[m] + zr[piece, m].astype(jnp.float32)
            mixed_ref[m, :, piece * tile_w : (piece + 1) * tile_w] = (
                both * gating_ref[m, :, 0:1]
            ).astype(jnp.bfloat16)
    for copy in pending:
        copy.wait_send()


def on_device(tokens, modality, routes, router, w_in, w_out):
    micro, tok, width = tokens.shape
    experts = router.shape[1]
    cap = 2 * tok // experts
    ranks = lax.axis_size("dp")
    group = ranks // 4
    total = experts * ranks
    half_ff = w_in.shape[2] // 2
    tile_w = 256 if width % 256 == 0 else 128
    pieces = width // tile_w

    pad = -(-experts // 8) * 8
    router_rows = jnp.pad(router.T, ((0, pad - experts), (0, 0)))

    bf16 = jnp.bfloat16
    dma = pltpu.SemaphoreType.DMA
    vmem = pl.BlockSpec(memory_space=pltpu.VMEM)
    mixed, summed = pl.pallas_call(
        functools.partial(layer_kernel, experts, ranks),
        out_shape=(
            jax.ShapeDtypeStruct(tokens.shape, bf16),
            jax.ShapeDtypeStruct((pad, 128), jnp.float32),
        ),
        in_specs=[vmem] * 6,
        out_specs=(vmem, vmem),
        scratch_shapes=[
            pltpu.VMEM((micro, tok, width), bf16),
            pltpu.VMEM((micro, 8, tok), jnp.int32),
            pltpu.VMEM((total, pad, 128), jnp.float32),
            pltpu.VMEM((width, half_ff), bf16),
            pltpu.VMEM((half_ff, width), bf16),
            pltpu.VMEM((2, experts, micro, cap, width), bf16),
            pltpu.VMEM((2, experts, micro, cap, width), bf16),
            pltpu.VMEM((2, experts * micro * cap, half_ff), jnp.float32),
            pltpu.VMEM((2, experts * micro * cap, half_ff), bf16),
            pltpu.VMEM((2, pieces, experts, micro, cap, tile_w), bf16),
            pltpu.VMEM((2, pieces, experts, micro, cap, tile_w), bf16),
            pltpu.VMEM((pieces, micro, tok, tile_w), bf16),
            pltpu.VMEM((pieces, micro, tok, tile_w), bf16),
            pltpu.VMEM((micro, 8, tok), jnp.int32),
            pltpu.VMEM((micro, tok, tok), jnp.float32),
            pltpu.VMEM((pad, 128), jnp.float32),
            dma((2,)),
            dma((2,)),
            dma((2,)),
            dma((2, 2, 2, group)),
            dma((2, pieces, 2, group)),
            dma((2, 2, experts)),
            dma((2, 2, pieces, experts)),
            dma((2, pieces)),
        ],
        compiler_params=pltpu.CompilerParams(
            collective_id=0, has_side_effects=True, vmem_limit_bytes=64 * 1024 * 1024 - 65536
        ),
    )(tokens, routes[:, :, 0], modality, router_rows, w_in[0], w_out[0])

    load = summed[:experts, :4].T.reshape(2, 2, experts)
    return (mixed, load)


def solution(mesh):
    placed = (
        P(None, ("expert", "dp"), None),
        P(None, ("expert", "dp")),
        P(None, ("expert", "dp"), None),
        P(),
        P("expert", "dp", None),
        P("expert", "dp", None),
    )
    return jax.shard_map(
        on_device,
        mesh=mesh,
        in_specs=placed,
        out_specs=(P(None, ("expert", "dp"), None), P()),
        check_vma=False,
    )
```
